32 devices in a mesh: dp: 8 (over z, x), feat: 4 (over y, core).
Axes of the slice: x: 2, y: 2, z: 4, core: 2. Of those that a mesh axis runs over, the one named last changes fastest.
Arguments:
- features: float32 [24576, 2048], P('dp', 'feat'), may hold values from -200 to 200
- gamma: float32 [2048], P('feat'), may hold values from 0.5 to 1.5
- beta: float32 [2048], P('feat'), may hold values from -3 to 3
- weight: bfloat16 [2048, 2048], P(None, 'feat'), may hold values from -0.125 to 0.125
- bias: float32 [2048], P('feat'), may hold values from -3 to 3
Outputs:
- activated: float32 [24576, 2048], P('dp', 'feat')
The draws below stay inside these ranges and needn't reach their ends.
All inputs are finite; a program needn't handle non-finite values.
Results may differ from the reference program's by a relative error of at most 0.0026.
Values may be sent and summed in bfloat16 or wider, within the bound.
No kernel may reach another device: no remote copies, remote signals or barrier semaphores. Data moves between devices by JAX's collectives and lax.ppermute only.
A program may use at most 128 MiB of HBM per device.

```python
import jax
import jax.numpy as jnp
from jax import lax

F = 2048
ROWS_DEV = 3072
ROWS = 24576


def draw_features(key, part):
    key_noise = jax.random.fold_in(key, 11)
    key_feat = jax.random.fold_in(key, 12)
    key_sign = jax.random.fold_in(key, 13)
    blocks = ROWS // ROWS_DEV
    block = (jnp.arange(ROWS) // ROWS_DEV).astype(jnp.float32)
    rising = block / max(blocks - 1, 1)
    block_scale = 3.0 ** rising
    feat_scale = jnp.exp(jax.random.uniform(key_feat, (F,), jnp.float32, 0.0, 2.0) - 0.7)
    feat_sign = jax.random.normal(key_sign, (F,), jnp.float32)
    offset = (2.0 * rising - 1.0)[:, None] * feat_sign[None, :]
    noise = jax.random.normal(key_noise, (ROWS, F), jnp.float32)
    values = offset + noise * feat_scale[None, :] * block_scale[:, None]
    return jnp.clip(values, -200.0, 200.0)


def shard_levels(key, shape, split, smallest, high):
    def one(dim, shards_of):
        draws = jax.random.uniform(jax.random.fold_in(jax.random.fold_in(key, 6), dim), (shards_of,), jnp.float32, smallest / len(split), high / len(split))
        return jnp.repeat(jnp.exp(draws), shape[dim] // shards_of).reshape((-1,) + (1,) * (len(shape) - dim - 1))

    factor_of = one(*split[0])
    for cut in split[1:]:
        factor_of = factor_of * one(*cut)
    return factor_of


def bell_draw(stream_key, extent, spread, most, shards=(), dtype=jnp.bfloat16):
    loudness = shard_levels(stream_key, extent, shards, -0.22, 0.18) if shards else 1.0
    result = jax.random.normal(stream_key, extent, jnp.float32) * spread * loudness
    return jnp.minimum(jnp.maximum(result, -most), most).astype(dtype)


def setup_inputs(seed: int = 0) -> dict:
    seeds = jax.random.split(jax.random.key(seed), 6)
    features = draw_features(jax.random.fold_in(seeds[5], 71), 0)
    gamma = jnp.clip(1.0 + 0.1 * jax.random.normal(seeds[1], (F,), jnp.float32), 0.5, 1.5)
    beta = bell_draw(seeds[2], (F,), 0.5, 3.0, ((0, 4),), jnp.float32)
    weight = bell_draw(seeds[3], (F, F), F ** -0.5, 0.125, ((1, 4),))
    bias = bell_draw(seeds[4], (F,), 0.5, 3.0, ((0, 4),), jnp.float32)
    return dict(features=features, gamma=gamma, beta=beta, weight=weight, bias=bias)


def reference(features, gamma, beta, weight, bias):
    mean = lax.optimization_barrier(jnp.mean(features, axis=0))
    centred = features - mean
    var = lax.optimization_barrier(jnp.mean(centred * centred, axis=0))
    scale = gamma / jnp.sqrt(var + 1e-05)
    normed = (centred * scale + beta).astype(jnp.bfloat16)
    product = jnp.dot(normed, weight, preferred_element_type=jnp.float32)
    return jnp.maximum(product + bias, 0.0)
```

```python
import functools

import jax
import jax.numpy as jnp
from jax import lax
from jax.experimental import pallas as pl
from jax.experimental.pallas import tpu as pltpu
from jax.sharding import PartitionSpec as P


UNITS = 24
EARLY = (2, 4)
LATE = (6, 6, 4, 1, 1)


def centre_kernel(x_ref, sent_ref, mean_ref, dev_ref):
    b = pl.program_id(0)
    x = x_ref[...]
    mean = jnp.mean(x, axis=0, keepdims=True)
    d = x - mean
    sent_ref[...] = d.astype(jnp.bfloat16)
    mean_ref[pl.ds(b, 1), :] = mean
    dev_ref[pl.ds(b, 1), :] = jnp.sum(d * d, axis=0, keepdims=True)


def centre(features, first, count, unit):
    cols = features.shape[1]
    pad = -(-count // 8) * 8
    sent, mean, dev = pl.pallas_call(
        centre_kernel,
        grid=(count,),
        in_specs=[pl.BlockSpec((unit, cols), lambda b: (b + first, 0))],
        out_specs=[
            pl.BlockSpec((unit, cols), lambda b: (b, 0)),
            pl.BlockSpec((pad, cols), lambda b: (0, 0)),
            pl.BlockSpec((pad, cols), lambda b: (0, 0)),
        ],
        out_shape=[
            jax.ShapeDtypeStruct((count * unit, cols), jnp.bfloat16),
            jax.ShapeDtypeStruct((pad, cols), jnp.float32),
            jax.ShapeDtypeStruct((pad, cols), jnp.float32),
        ],
        name=f"centre{first}",
    )(features)
    return sent, mean[:count], dev[:count]


def moments_kernel(x_ref, mean_ref, dev_ref, *, unit, per):
    b = pl.program_id(0)
    for u in range(per):
        x = x_ref[pl.ds(u * unit, unit), :]
        mean = jnp.mean(x, axis=0, keepdims=True)
        d = x - mean
        mean_ref[pl.ds(b * per + u, 1), :] = mean
        dev_ref[pl.ds(b * per + u, 1), :] = jnp.sum(d * d, axis=0, keepdims=True)


def moments(features, first, count, unit):
    cols = features.shape[1]
    per = first
    while count % per or first % per:
        per -= 1
    pad = -(-count // 8) * 8
    mean, dev = pl.pallas_call(
        functools.partial(moments_kernel, unit=unit, per=per),
        grid=(count // per,),
        in_specs=[pl.BlockSpec((per * unit, cols), lambda b: (b + first // per, 0))],
        out_specs=[
            pl.BlockSpec((pad, cols), lambda b: (0, 0)),
            pl.BlockSpec((pad, cols), lambda b: (0, 0)),
        ],
        out_shape=[
            jax.ShapeDtypeStruct((pad, cols), jnp.float32),
            jax.ShapeDtypeStruct((pad, cols), jnp.float32),
        ],
        name="moments",
    )(features)
    return mean[:count], dev[:count]


def matmul_kernel(place, *refs, shards, aliased):
    xs = refs[:shards]
    ws = refs[shards : 2 * shards]
    bias_ref = refs[2 * shards]
    out_ref = refs[-1]
    total = bias_ref[...]
    for x, w in zip(xs, ws):
        total = total + jnp.dot(x[...], w[...], preferred_element_type=jnp.float32)
    out_ref[...] = jnp.maximum(total, 0.0)


def matmul(xs, order, weight, bias, out, first, rows):
    shards = len(xs)
    count, cols = xs[0].shape
    width = weight.shape[1]
    block = min(count, 512)
    while count % block or first % block:
        block -= 8
    offset = first // block
    in_specs = [pl.BlockSpec((block, cols), lambda i, s: (i, 0)) for _ in range(shards)]
    in_specs += [pl.BlockSpec((cols, width), functools.partial(lambda j, i, s: (s[j], 0), j)) for j in range(shards)]
    in_specs += [pl.BlockSpec((1, width), lambda i, s: (0, 0))]
    args = [order, *xs, *([weight] * shards), bias]
    aliases = {}
    if out is not None:
        in_specs += [pl.BlockSpec(memory_space=pl.ANY)]
        aliases = {len(args): 0}
        args += [out]
    return pl.pallas_call(
        functools.partial(matmul_kernel, shards=shards, aliased=out is not None),
        grid_spec=pltpu.PrefetchScalarGridSpec(
            num_scalar_prefetch=1,
            grid=(count // block,),
            in_specs=in_specs,
            out_specs=pl.BlockSpec((block, width), lambda i, s: (i + offset, 0)),
        ),
        out_shape=jax.ShapeDtypeStruct((rows, width), jnp.float32),
        input_output_aliases=aliases,
        name=f"layer{first}",
    )(*args)


def local(features, gamma, beta, weight, bias):
    rows, cols = features.shape
    dp = lax.axis_size("dp")
    feat = lax.axis_size("feat")
    unit = rows // UNITS
    total_rows = rows * dp
    me = lax.axis_index("feat")
    near = [(i, i ^ 1) for i in range(feat)]
    shifts = range(2, feat, 2)
    far = {s: [(i, (i + s) % feat) for i in range(feat)] for s in shifts}

    def to_far(x):
        return [lax.ppermute(x, "feat", far[s]) for s in shifts]

    def to_near(x):
        return lax.ppermute(x, "feat", near)

    order = [me, me ^ 1]
    for s in shifts:
        source = (me - s) % feat
        order += [source, source ^ 1]
    order = jnp.stack(order).astype(jnp.int32)

    means, devs, early = [], [], []
    first = 0
    for count in EARLY:
        sent, mean, dev = centre(features, first, count, unit)
        means.append(mean)
        devs.append(dev)
        early.append((first, count, to_far(sent)))
        first += count
    mean, dev = moments(features, first, UNITS - first, unit)
    unit_means = jnp.concatenate(means + [mean])
    unit_devs = jnp.concatenate(devs + [dev])
    mean = jnp.mean(unit_means, axis=0)
    gaps = unit_means - mean
    dev = jnp.sum(unit_devs, axis=0) + unit * jnp.sum(gaps * gaps, axis=0)
    step, held = 1, rows
    while step < dp:
        mine = jnp.stack([mean, dev])
        theirs = lax.ppermute(mine, "dp", [(i, i ^ step) for i in range(dp)])
        gap = mean - theirs[0]
        mean = (mean + theirs[0]) * 0.5
        dev = dev + theirs[1] + (0.5 * held) * (gap * gap)
        step, held = 2 * step, 2 * held
    var = dev / total_rows
    scale = gamma / jnp.sqrt(var + 1e-05)

    def normalize(first, count):
        x = features[first * unit : (first + count) * unit]
        return ((x - mean) * scale + beta).astype(jnp.bfloat16)

    firsts = (unit_means[: sum(EARLY)] - mean) * scale + beta
    table = to_far(jnp.concatenate([scale[None], firsts]))
    parts = []
    for start, count, arrived in early:
        own = normalize(start, count)
        fixed = []
        for got, t in zip(arrived, table):
            got = got.reshape(count, unit, cols).astype(jnp.float32)
            got = got * t[0] + t[1 + start : 1 + start + count][:, None, :]
            fixed.append(got.astype(jnp.bfloat16).reshape(count * unit, cols))
        parts.append((start, own, fixed))
    for count in LATE:
        own = normalize(first, count)
        parts.append((first, own, to_far(own)))
        first += count

    out = None
    for start, own, arrived in parts:
        xs = [own, to_near(own)]
        for got in arrived:
            xs += [got, to_near(got)]
        out = matmul(xs, order, weight, bias[None], out, start * unit, rows)
    return out


def solution(mesh):
    placed = (P("dp", "feat"), P("feat"), P("feat"), P(None, "feat"), P("feat"))
    return jax.shard_map(
        local, mesh=mesh, in_specs=placed, out_specs=P("dp", "feat"), check_vma=False
    )
```

```python
import functools

import jax
import jax.numpy as jnp
from jax import lax
from jax.experimental import pallas as pl
from jax.experimental.pallas import tpu as pltpu
from jax.sharding import PartitionSpec as P


UNITS = 24
EARLY = (2, 8)
LATE = (6, 4, 3, 1)


def grant(kib):
    return pltpu.CompilerParams(vmem_limit_bytes=kib * 1024)


def block_of(first, count, most):
    per = min(count, most)
    while count % per or first % per:
        per -= 1
    return per


def centre_kernel(x_ref, sent_ref, mean_ref, dev_ref):
    b = pl.program_id(0)
    x = x_ref[...]
    mean = jnp.mean(x, axis=0, keepdims=True)
    d = x - mean
    sent_ref[...] = d.astype(jnp.bfloat16)
    mean_ref[pl.ds(b, 1), :] = mean
    dev_ref[pl.ds(b, 1), :] = jnp.sum(d * d, axis=0, keepdims=True)


def centre(features, first, count, unit):
    cols = features.shape[1]
    per = block_of(first, count, 4)
    blocks = count // per
    return pl.pallas_call(
        centre_kernel,
        grid=(blocks,),
        in_specs=[pl.BlockSpec((per * unit, cols), lambda b: (b + first // per, 0))],
        out_specs=[
            pl.BlockSpec((per * unit, cols), lambda b: (b, 0)),
            pl.BlockSpec((blocks, cols), lambda b: (0, 0)),
            pl.BlockSpec((blocks, cols), lambda b: (0, 0)),
        ],
        out_shape=[
            jax.ShapeDtypeStruct((count * unit, cols), jnp.bfloat16),
            jax.ShapeDtypeStruct((blocks, cols), jnp.float32),
            jax.ShapeDtypeStruct((blocks, cols), jnp.float32),
        ],
        compiler_params=grant(8192),
    )(features)


def moments_kernel(x_ref, *refs, sizes, rest):
    early, (total_ref, sum_ref, dev_ref) = refs[: 2 * len(sizes)], refs[2 * len(sizes) :]
    b = pl.program_id(0)
    pivot = early[0][0:1, :]
    d = x_ref[...] - pivot
    d = d.reshape(-1, 8, d.shape[1])

    @pl.when(b == 0)
    def _():
        sum_ref[...] = jnp.zeros_like(sum_ref)
        dev_ref[...] = jnp.zeros_like(dev_ref)

    sum_ref[...] += jnp.sum(d, axis=0)
    dev_ref[...] += jnp.sum(d * d, axis=0)

    @pl.when(b == pl.num_programs(0) - 1)
    def _():
        shift = jnp.sum(sum_ref[...], axis=0, keepdims=True) / rest
        dev = jnp.sum(dev_ref[...], axis=0, keepdims=True) - rest * (shift * shift)
        groups = [(rest, pivot + shift, dev)]
        for n, m, d in zip(sizes, early[::2], early[1::2]):
            for r in range(m.shape[0]):
                groups.append((n, m[r : r + 1, :], d[r : r + 1, :]))
        rows = sum(n for n, _, _ in groups)
        mean = sum(n * m for n, m, _ in groups) / rows
        dev = sum(d + n * ((m - mean) * (m - mean)) for n, m, d in groups)
        total_ref[0:1, :] = mean
        total_ref[1:2, :] = dev


def moments(features, first, count, unit, early, sizes):
    cols = features.shape[1]
    per = block_of(first, count, 4)
    flat = [a for pair in early for a in pair]
    return pl.pallas_call(
        functools.partial(moments_kernel, sizes=sizes, rest=count * unit),
        grid=(count // per,),
        in_specs=[pl.BlockSpec((per * unit, cols), lambda b: (b + first // per, 0))]
        + [pl.BlockSpec(a.shape, lambda b: (0, 0)) for a in flat],
        out_specs=pl.BlockSpec((2, cols), lambda b: (0, 0)),
        out_shape=jax.ShapeDtypeStruct((2, cols), jnp.float32),
        scratch_shapes=[pltpu.VMEM((8, cols), jnp.float32)] * 2,
        compiler_params=grant(8192),
    )(features, *flat)


def shard_order():
    feat = lax.axis_size("feat")
    me = lax.axis_index("feat")
    order = [me, me ^ 1]
    for s in range(2, feat, 2):
        source = (me - s) % feat
        order += [source, source ^ 1]
    return order


def layer_kernel(*refs, shards):
    xs = refs[:shards]
    w_ref, bias_ref = refs[shards : shards + 2]
    out_ref = refs[-1]
    cols = xs[0].shape[1]
    total = bias_ref[...]
    for x, shard in zip(xs, shard_order()):
        start = pl.multiple_of(shard * cols, cols)
        total = total + jnp.dot(x[...], w_ref[pl.ds(start, cols), :], preferred_element_type=jnp.float32)
    out_ref[...] = jnp.maximum(total, 0.0)


def layer(xs, weight, bias, out, first, rows, unit):
    shards = len(xs)
    count, cols = xs[0].shape
    width = weight.shape[1]
    block = block_of(first, count // unit, 4)
    offset = first // block
    block *= unit
    in_specs = [pl.BlockSpec((block, cols), lambda i: (i, 0)) for _ in range(shards)]
    in_specs += [pl.BlockSpec(memory_space=pltpu.VMEM)] * 2
    args = [*xs, weight, bias]
    aliases = {}
    if out is not None:
        in_specs += [pl.BlockSpec(memory_space=pl.ANY)]
        aliases = {len(args): 0}
        args += [out]
    return pl.pallas_call(
        functools.partial(layer_kernel, shards=shards),
        grid=(count // block,),
        in_specs=in_specs,
        out_specs=pl.BlockSpec((block, width), lambda i: (i + offset, 0)),
        out_shape=jax.ShapeDtypeStruct((rows, width), jnp.float32),
        input_output_aliases=aliases,
        compiler_params=grant(12288),
    )(*args)


def local(features, gamma, beta, weight, bias):
    rows, cols = features.shape
    dp = lax.axis_size("dp")
    feat = lax.axis_size("feat")
    unit = rows // UNITS
    total_rows = rows * dp
    near = [(i, i ^ 1) for i in range(feat)]
    shifts = range(2, feat, 2)

    def to_far(x):
        return [lax.ppermute(x, "feat", [(i, (i + s) % feat) for i in range(feat)]) for s in shifts]

    def to_near(x):
        return lax.ppermute(x, "feat", near)

    early, found, sizes, firsts = [], [], [], [0]
    for count in EARLY + LATE:
        firsts.append(firsts[-1] + count)
    for k, count in enumerate(EARLY):
        sent, mean, dev = centre(features, firsts[k], count, unit)
        early.append(to_far(sent))
        found.append((mean, dev))
        sizes.append(count * unit // mean.shape[0])
    ahead = firsts[len(EARLY)]
    mine = moments(features, ahead, UNITS - ahead, unit, found, tuple(sizes))
    step, held = 1, rows
    while step < dp:
        theirs = lax.ppermute(mine, "dp", [(i, i ^ step) for i in range(dp)])
        gap = mine[0] - theirs[0]
        mean = (mine[0] + theirs[0]) * 0.5
        dev = mine[1] + theirs[1] + (0.5 * held) * (gap * gap)
        mine = jnp.stack([mean, dev])
        step, held = 2 * step, 2 * held
    mean = mine[0]
    var = mine[1] / total_rows
    scale = gamma / jnp.sqrt(var + 1e-05)

    def normalize(k):
        x = features[firsts[k] * unit : firsts[k + 1] * unit]
        return ((x - mean) * scale + beta).astype(jnp.bfloat16)

    own, arrived = {}, {}
    for k in range(len(EARLY), len(EARLY) + len(LATE)):
        own[k] = normalize(k)
        arrived[k] = to_far(own[k])
    offsets = (jnp.concatenate([m for m, _ in found]) - mean) * scale + beta
    table = to_far(jnp.concatenate([scale[None], offsets]))
    row = 1
    for k, (mean_of, _) in enumerate(found):
        own[k] = normalize(k)
        arrived[k] = []
        blocks = mean_of.shape[0]
        for got, t in zip(early[k], table):
            got = got.reshape(blocks, sizes[k], cols).astype(jnp.float32)
            got = got * t[0] + t[row : row + blocks][:, None, :]
            arrived[k].append(got.astype(jnp.bfloat16).reshape(blocks * sizes[k], cols))
        row += blocks

    out = None
    for k in range(len(EARLY) + len(LATE)):
        xs = [own[k], to_near(own[k])]
        for got in arrived[k]:
            xs += [got, to_near(got)]
        out = layer(xs, weight, bias[None], out, firsts[k], rows, unit)
    return out


def solution(mesh):
    placed = (P("dp", "feat"), P("feat"), P("feat"), P(None, "feat"), P("feat"))
    return jax.shard_map(
        local, mesh=mesh, in_specs=placed, out_specs=P("dp", "feat"), check_vma=False
    )
```

```python
import functools

import jax
import jax.numpy as jnp
from jax import lax
from jax.experimental import pallas as pl
from jax.experimental.pallas import tpu as pltpu
from jax.sharding import PartitionSpec as P


UNITS = 24
EARLY = (2, 6)
LATE = (7, 4, 3, 1, 1)
PIECE = 2
SPLIT = 3


def grant(kib):
    return pltpu.CompilerParams(vmem_limit_bytes=kib * 1024)


def centred(x):
    mean = jnp.mean(x, axis=0, keepdims=True)
    d = x - mean
    return d.astype(jnp.bfloat16), mean, jnp.sum(d * d, axis=0, keepdims=True)


def centre_kernel(x_ref, sent_ref, stat_ref, buf, sem):
    copy = pltpu.make_async_copy(x_ref.at[pl.ds(0, buf.shape[0]), :], buf, sem)
    copy.start()
    copy.wait()
    sent, mean, dev = centred(buf[...])
    sent_ref[...] = sent
    stat_ref[0:1, :] = mean
    stat_ref[1:2, :] = dev


def centre(features, count):
    cols = features.shape[1]
    return pl.pallas_call(
        centre_kernel,
        in_specs=[pl.BlockSpec(memory_space=pltpu.HBM)],
        out_specs=[pl.BlockSpec(memory_space=pltpu.VMEM)] * 2,
        out_shape=[
            jax.ShapeDtypeStruct((count, cols), jnp.bfloat16),
            jax.ShapeDtypeStruct((2, cols), jnp.float32),
        ],
        scratch_shapes=[pltpu.VMEM((count, cols), jnp.float32), pltpu.SemaphoreType.DMA],
        compiler_params=grant(51000),
    )(features)


def survey_kernel(x_ref, stat_ref, held_ref, sent_ref, means_ref, total_ref, sems, *, first, early, piece):
    rows, cols = held_ref.shape
    pieces = rows // piece
    order = [p for p in range(pieces) if p * piece >= first] + [p for p in range(pieces) if p * piece < first]
    copies = {}
    for p in order:
        place = pl.ds(p * piece, piece)
        copies[p] = pltpu.make_async_copy(x_ref.at[place, :], held_ref.at[place, :], sems.at[p])
        copies[p].start()
    pivot = stat_ref[0:1, :]
    groups = [(first, pivot, stat_ref[1:2, :])]
    sums = jnp.zeros((8, cols), jnp.float32)
    devs = jnp.zeros((8, cols), jnp.float32)
    rest = 0
    for p in order:
        copies[p].wait()
        if p * piece < first:
            continue
        x = held_ref[pl.ds(p * piece, piece), :]
        if p * piece < first + early:
            sent, mean, dev = centred(x)
            sent_ref[pl.ds(p * piece - first, piece), :] = sent
            means_ref[pl.ds(p - first // piece, 1), :] = mean
            groups.append((piece, mean, dev))
        else:
            d = (x - pivot).reshape(-1, 8, cols)
            sums = sums + jnp.sum(d, axis=0)
            devs = devs + jnp.sum(d * d, axis=0)
            rest += piece
    shift = jnp.sum(sums, axis=0, keepdims=True) / rest
    dev = jnp.sum(devs, axis=0, keepdims=True) - rest * (shift * shift)
    groups.append((rest, pivot + shift, dev))
    mean = sum(n * m for n, m, _ in groups) / rows
    dev = sum(d + n * ((m - mean) * (m - mean)) for n, m, d in groups)
    total_ref[0:1, :] = mean
    total_ref[1:2, :] = dev


def survey(features, stat, first, early, piece):
    rows, cols = features.shape
    return pl.pallas_call(
        functools.partial(survey_kernel, first=first, early=early, piece=piece),
        in_specs=[pl.BlockSpec(memory_space=pltpu.HBM), pl.BlockSpec(memory_space=pltpu.VMEM)],
        out_specs=[pl.BlockSpec(memory_space=pltpu.VMEM)] * 4,
        out_shape=[
            jax.ShapeDtypeStruct((rows, cols), jnp.float32),
            jax.ShapeDtypeStruct((early, cols), jnp.bfloat16),
            jax.ShapeDtypeStruct((early // piece, cols), jnp.float32),
            jax.ShapeDtypeStruct((2, cols), jnp.float32),
        ],
        scratch_shapes=[pltpu.SemaphoreType.DMA((rows // piece,))],
        compiler_params=grant(46000),
    )(features, stat)


def shard_order():
    feat = lax.axis_size("feat")
    me = lax.axis_index("feat")
    order = [me, me ^ 1]
    for s in range(2, feat, 2):
        source = (me - s) % feat
        order += [source, source ^ 1]
    return order


def product(xs, places, w_ref, total, rows):
    cols = xs[0].shape[1]
    order = shard_order()
    for x, place in zip(xs, places):
        start = pl.multiple_of(order[place] * cols, cols)
        w = w_ref[pl.ds(start, cols), :]
        total = total + jnp.dot(x[rows, :], w, preferred_element_type=jnp.float32)
    return total


def part_kernel(*refs, places):
    n = len(places)
    xs, (w_ref, bias_ref, out_ref) = refs[:n], refs[n:]
    out_ref[...] = product(xs, places, w_ref, bias_ref[...], pl.ds(0, xs[0].shape[0]))


def part(xs, places, weight, bias):
    return pl.pallas_call(
        functools.partial(part_kernel, places=places),
        in_specs=[pl.BlockSpec(memory_space=pltpu.VMEM)] * (len(xs) + 2),
        out_specs=pl.BlockSpec(memory_space=pltpu.VMEM),
        out_shape=jax.ShapeDtypeStruct((xs[0].shape[0], weight.shape[1]), jnp.float32),
        compiler_params=grant(12288),
    )(*xs, weight, bias)


def layer_kernel(*refs, places, first, block):
    n = len(places)
    xs, (w_ref, base_ref) = refs[:n], refs[n : n + 2]
    out_ref, buf, sems = refs[-3:]
    copies = []
    for b in range(xs[0].shape[0] // block):
        rows = pl.ds(b * block, block)
        base = base_ref[...] if base_ref.shape[0] == 1 else base_ref[rows, :]
        buf[rows, :] = jnp.maximum(product(xs, places, w_ref, base, rows), 0.0)
        copies.append(
            pltpu.make_async_copy(buf.at[rows, :], out_ref.at[pl.ds(first + b * block, block), :], sems.at[b])
        )
        copies[-1].start()
    for copy in copies:
        copy.wait()


def layer(xs, places, weight, base, out, first, rows, unit):
    count = xs[0].shape[0]
    width = weight.shape[1]
    block = 2 * unit if count % (2 * unit) == 0 else unit
    in_specs = [pl.BlockSpec(memory_space=pltpu.VMEM)] * (len(xs) + 2)
    args = [*xs, weight, base]
    aliases = {}
    if out is not None:
        in_specs += [pl.BlockSpec(memory_space=pltpu.HBM)]
        aliases = {len(args): 0}
        args += [out]
    return pl.pallas_call(
        functools.partial(layer_kernel, places=places, first=first, block=block),
        in_specs=in_specs,
        out_specs=pl.BlockSpec(memory_space=pltpu.HBM),
        out_shape=jax.ShapeDtypeStruct((rows, width), jnp.float32),
        input_output_aliases=aliases,
        scratch_shapes=[pltpu.VMEM((count, width), jnp.float32), pltpu.SemaphoreType.DMA((count // block,))],
        compiler_params=grant(12288),
    )(*args)


def local(features, gamma, beta, weight, bias):
    rows, cols = features.shape
    dp = lax.axis_size("dp")
    feat = lax.axis_size("feat")
    unit = rows // UNITS
    total_rows = rows * dp
    near = [(i, i ^ 1) for i in range(feat)]
    shifts = range(2, feat, 2)

    def to_far(x):
        return [lax.ppermute(x, "feat", [(i, (i + s) % feat) for i in range(feat)]) for s in shifts]

    def to_near(x):
        return lax.ppermute(x, "feat", near)

    firsts = [0]
    for count in EARLY + LATE:
        firsts.append(firsts[-1] + count)
    piece = PIECE * unit
    sizes = [EARLY[0] * unit, piece]
    sent, stat = centre(features, EARLY[0] * unit)
    early = [to_far(sent)]
    features, sent, means, mine = survey(features, stat, EARLY[0] * unit, EARLY[1] * unit, piece)
    early.append(to_far(sent))
    found = [stat[:1], means]
    step, held = 1, rows
    while step < dp:
        theirs = lax.ppermute(mine, "dp", [(i, i ^ step) for i in range(dp)])
        gap = mine[0] - theirs[0]
        mean = (mine[0] + theirs[0]) * 0.5
        dev = mine[1] + theirs[1] + (0.5 * held) * (gap * gap)
        mine = jnp.stack([mean, dev])
        step, held = 2 * step, 2 * held
    mean = mine[0]
    var = mine[1] / total_rows
    scale = gamma / jnp.sqrt(var + 1e-05)

    def normalize(k):
        x = features[firsts[k] * unit : firsts[k + 1] * unit]
        return ((x - mean) * scale + beta).astype(jnp.bfloat16)

    own, arrived = {}, {}
    for k in range(len(EARLY), len(EARLY) + len(LATE)):
        own[k] = normalize(k)
        arrived[k] = to_far(own[k])
    offsets = (jnp.concatenate(found) - mean) * scale + beta
    table = to_far(jnp.concatenate([scale[None], offsets]))
    row = 1
    for k, means in enumerate(found):
        own[k] = normalize(k)
        arrived[k] = []
        blocks = means.shape[0]
        for got, t in zip(early[k], table):
            got = got.reshape(blocks, sizes[k], cols).astype(jnp.float32)
            got = got * t[0] + t[row : row + blocks][:, None, :]
            arrived[k].append(got.astype(jnp.bfloat16).reshape(blocks * sizes[k], cols))
        row += blocks

    out = None
    bias = bias[None]
    for k in range(len(EARLY) + len(LATE)):
        xs = [own[k], to_near(own[k])]
        for got in arrived[k]:
            xs += [got, to_near(got)]
        places = tuple(range(len(xs)))
        base = bias
        if k >= len(EARLY) + len(LATE) - SPLIT:
            passed = places[3::2]
            held = tuple(p for p in places if p not in passed)
            base = part([xs[p] for p in held], held, weight, bias)
            places, xs = passed, [xs[p] for p in passed]
        out = layer(xs, places, weight, base, out, firsts[k] * unit, rows, unit)
    return out


def solution(mesh):
    placed = (P("dp", "feat"), P("feat"), P("feat"), P(None, "feat"), P("feat"))
    return jax.shard_map(local, mesh=mesh, in_specs=placed, out_specs=P("dp", "feat"), check_vma=False)
```

```python
import functools

import jax
import jax.numpy as jnp
from jax import lax
from jax.experimental import pallas as pl
from jax.experimental.pallas import tpu as pltpu
from jax.sharding import PartitionSpec as P


UNITS = 96
EARLY = (8, 24)
LATE = (28, 16, 9, 5, 4)
DIRECT = 2
PIECE = 12
SPLIT = 3


def grant(kib):
    return pltpu.CompilerParams(vmem_limit_bytes=kib * 1024)


def centre_kernel(x_ref, sent_ref, mean_ref, buf, sem):
    copy = pltpu.make_async_copy(x_ref.at[pl.ds(0, buf.shape[0]), :], buf, sem)
    copy.start()
    copy.wait()
    x = buf[...]
    mean = jnp.mean(x, axis=0, keepdims=True)
    sent_ref[...] = (x - mean).astype(jnp.bfloat16)
    mean_ref[...] = mean


def centre(features, count):
    cols = features.shape[1]
    return pl.pallas_call(
        centre_kernel,
        in_specs=[pl.BlockSpec(memory_space=pltpu.HBM)],
        out_specs=[pl.BlockSpec(memory_space=pltpu.VMEM)] * 2,
        out_shape=[
            jax.ShapeDtypeStruct((count, cols), jnp.bfloat16),
            jax.ShapeDtypeStruct((1, cols), jnp.float32),
        ],
        scratch_shapes=[pltpu.VMEM((count, cols), jnp.float32), pltpu.SemaphoreType.DMA],
        compiler_params=grant(51000),
    )(features)


def survey_kernel(x_ref, pivot_ref, held_ref, sent_ref, means_ref, total_ref, sems, *, early, others):
    rows, cols = held_ref.shape
    copies = []
    for p, (start, size) in enumerate(early + others):
        place = pl.ds(start, size)
        copies.append(pltpu.make_async_copy(x_ref.at[place, :], held_ref.at[place, :], sems.at[p]))
        copies[-1].start()
    pivot = pivot_ref[...]
    groups = []
    for p, (start, size) in enumerate(early):
        copies[p].wait()
        x = held_ref[pl.ds(start, size), :]
        mean = jnp.mean(x, axis=0, keepdims=True)
        d = x - mean
        sent_ref[pl.ds(start - early[0][0], size), :] = d.astype(jnp.bfloat16)
        means_ref[pl.ds(p, 1), :] = mean
        groups.append((size, mean, jnp.sum(d * d, axis=0, keepdims=True)))
    sums = jnp.zeros((8, cols), jnp.float32)
    devs = jnp.zeros((8, cols), jnp.float32)
    rest = 0
    for p, (start, size) in enumerate(others, len(early)):
        copies[p].wait()
        d = (held_ref[pl.ds(start, size), :] - pivot).reshape(-1, 8, cols)
        sums = sums + jnp.sum(d, axis=0)
        devs = devs + jnp.sum(d * d, axis=0)
        rest += size
    shift = jnp.sum(sums, axis=0, keepdims=True) / rest
    dev = jnp.sum(devs, axis=0, keepdims=True) - rest * (shift * shift)
    groups.append((rest, pivot + shift, dev))
    mean = sum(n * m for n, m, _ in groups) / rows
    dev = sum(d + n * ((m - mean) * (m - mean)) for n, m, d in groups)
    total_ref[0:1, :] = mean
    total_ref[1:2, :] = dev


def survey(features, pivot, first, early, piece):
    rows, cols = features.shape
    pieces = tuple((first + p, piece) for p in range(0, early, piece))
    others = tuple((p, min(2 * piece, rows - p)) for p in range(first + early, rows, 2 * piece)) + ((0, first),)
    return pl.pallas_call(
        functools.partial(survey_kernel, early=pieces, others=others),
        in_specs=[pl.BlockSpec(memory_space=pltpu.HBM), pl.BlockSpec(memory_space=pltpu.VMEM)],
        out_specs=[pl.BlockSpec(memory_space=pltpu.VMEM)] * 4,
        out_shape=[
            jax.ShapeDtypeStruct((rows, cols), jnp.float32),
            jax.ShapeDtypeStruct((early, cols), jnp.bfloat16),
            jax.ShapeDtypeStruct((early // piece, cols), jnp.float32),
            jax.ShapeDtypeStruct((2, cols), jnp.float32),
        ],
        scratch_shapes=[pltpu.SemaphoreType.DMA((len(pieces) + len(others),))],
        compiler_params=grant(46000),
    )(features, pivot)


def shard_order():
    feat = lax.axis_size("feat")
    me = lax.axis_index("feat")
    order = [me, me ^ 1]
    for s in range(2, feat, 2):
        source = (me - s) % feat
        order += [source, source ^ 1]
    return order


def weights_of(w_ref, place, cols):
    return w_ref[pl.ds(pl.multiple_of(shard_order()[place] * cols, cols), cols), :]


def product(xs, places, w_ref, total):
    for x, place in zip(xs, places):
        w = weights_of(w_ref, place, x.shape[1])
        total = total + jnp.dot(x, w, preferred_element_type=jnp.float32)
    return total


def part_kernel(*refs, places):
    n = len(places)
    xs, (w_ref, bias_ref, out_ref) = refs[:n], refs[n:]
    out_ref[...] = product([x[...] for x in xs], places, w_ref, bias_ref[...])


def part(xs, places, weight, bias):
    return pl.pallas_call(
        functools.partial(part_kernel, places=places),
        in_specs=[pl.BlockSpec(memory_space=pltpu.VMEM)] * (len(xs) + 2),
        out_specs=pl.BlockSpec(memory_space=pltpu.VMEM),
        out_shape=jax.ShapeDtypeStruct((xs[0].shape[0], weight.shape[1]), jnp.float32),
        compiler_params=grant(12288),
    )(*xs, weight, bias)


def layer_kernel(*refs, places, first, blocks):
    n = len(places)
    xs, (w_ref, base_ref) = refs[:n], refs[n : n + 2]
    out_ref, buf, sems = refs[-3:]
    copies = []
    for b, (start, size) in enumerate(blocks):
        rows = pl.ds(start, size)
        base = base_ref[...] if base_ref.shape[0] == 1 else base_ref[rows, :]
        buf[rows, :] = jnp.maximum(product([x[rows, :] for x in xs], places, w_ref, base), 0.0)
        copies.append(pltpu.make_async_copy(buf.at[rows, :], out_ref.at[pl.ds(first + start, size), :], sems.at[b]))
        copies[-1].start()
    for copy in copies:
        copy.wait()


def layer(xs, places, weight, base, out, first, rows):
    count = xs[0].shape[0]
    width = weight.shape[1]
    blocks = tuple((start, min(256, count - start)) for start in range(0, count, 256))
    in_specs = [pl.BlockSpec(memory_space=pltpu.VMEM)] * (len(xs) + 2)
    args = [*xs, weight, base]
    aliases = {}
    if out is not None:
        in_specs += [pl.BlockSpec(memory_space=pltpu.HBM)]
        aliases = {len(args): 0}
        args += [out]
    return pl.pallas_call(
        functools.partial(layer_kernel, places=places, first=first, blocks=blocks),
        in_specs=in_specs,
        out_specs=pl.BlockSpec(memory_space=pltpu.HBM),
        out_shape=jax.ShapeDtypeStruct((rows, width), jnp.float32),
        input_output_aliases=aliases,
        scratch_shapes=[pltpu.VMEM((count, width), jnp.float32), pltpu.SemaphoreType.DMA((len(blocks),))],
        compiler_params=grant(12288),
    )(*args)


def finish_kernel(*refs, shifts):
    passed, far, cross = refs[:shifts], refs[shifts : 2 * shifts], refs[2 * shifts : 3 * shifts]
    w_ref, base_ref, tail_ref, _, out_ref, buf, sem = refs[3 * shifts :]
    count = buf.shape[0]
    tail = product([x[...] for x in far], range(2, 2 + 2 * shifts, 2), w_ref, tail_ref[...])
    xs = [jnp.concatenate([p[...], c[...]]) for p, c in zip(passed, cross)]
    base = jnp.concatenate([base_ref[...], tail])
    buf[...] = jnp.maximum(product(xs, range(3, 3 + 2 * shifts, 2), w_ref, base), 0.0)
    copy = pltpu.make_async_copy(buf, out_ref.at[pl.ds(out_ref.shape[0] - count, count), :], sem)
    copy.start()
    copy.wait()


def finish(passed, far, cross, weight, base, tail, out):
    count = base.shape[0] + tail.shape[0]
    vmem = 3 * len(passed) + 3
    return pl.pallas_call(
        functools.partial(finish_kernel, shifts=len(passed)),
        in_specs=[pl.BlockSpec(memory_space=pltpu.VMEM)] * vmem + [pl.BlockSpec(memory_space=pltpu.HBM)],
        out_specs=pl.BlockSpec(memory_space=pltpu.HBM),
        out_shape=jax.ShapeDtypeStruct(out.shape, out.dtype),
        input_output_aliases={vmem: 0},
        scratch_shapes=[pltpu.VMEM((count, weight.shape[1]), jnp.float32), pltpu.SemaphoreType.DMA],
        compiler_params=grant(12288),
    )(*passed, *far, *cross, weight, base, tail, out)


def local(features, gamma, beta, weight, bias):
    rows, cols = features.shape
    dp = lax.axis_size("dp")
    feat = lax.axis_size("feat")
    unit = rows // UNITS
    total_rows = rows * dp
    near = [(i, i ^ 1) for i in range(feat)]
    shifts = range(2, feat, 2)

    def to_far(x):
        return [lax.ppermute(x, "feat", [(i, (i + s) % feat) for i in range(feat)]) for s in shifts]

    def to_cross(x):
        return [lax.ppermute(x, "feat", [(i, (i + s) % feat ^ 1) for i in range(feat)]) for s in shifts]

    def to_near(x):
        return lax.ppermute(x, "feat", near)

    firsts = [0]
    for count in EARLY + LATE + (DIRECT,):
        firsts.append(firsts[-1] + count)
    piece = PIECE * unit
    sizes = [EARLY[0] * unit, piece]
    sent, pivot = centre(features, EARLY[0] * unit)
    early = [to_far(sent)]
    features, sent, means, mine = survey(features, pivot, EARLY[0] * unit, EARLY[1] * unit, piece)
    early.append(to_far(sent))
    found = [pivot, means]
    step, held = 1, rows
    while step < dp:
        theirs = lax.ppermute(mine, "dp", [(i, i ^ step) for i in range(dp)])
        gap = mine[0] - theirs[0]
        mean = (mine[0] + theirs[0]) * 0.5
        dev = mine[1] + theirs[1] + (0.5 * held) * (gap * gap)
        mine = jnp.stack([mean, dev])
        step, held = 2 * step, 2 * held
    mean = mine[0]
    var = mine[1] / total_rows
    scale = gamma / jnp.sqrt(var + 1e-05)

    def normalize(k):
        x = features[firsts[k] * unit : firsts[k + 1] * unit]
        return ((x - mean) * scale + beta).astype(jnp.bfloat16)

    own, arrived = {}, {}
    last = len(EARLY) + len(LATE)
    for k in range(len(EARLY), last + 1):
        own[k] = normalize(k)
        arrived[k] = to_far(own[k])
    crossed = to_cross(own[last])
    offsets = (jnp.concatenate(found) - mean) * scale + beta
    table = to_far(jnp.concatenate([scale[None], offsets]))
    row = 1
    for k, means in enumerate(found):
        own[k] = normalize(k)
        arrived[k] = []
        blocks = means.shape[0]
        for got, t in zip(early[k], table):
            got = got.reshape(blocks, sizes[k], cols).astype(jnp.float32)
            got = got * t[0] + t[row : row + blocks][:, None, :]
            arrived[k].append(got.astype(jnp.bfloat16).reshape(blocks * sizes[k], cols))
        row += blocks

    out = None
    bias = bias[None]
    places = tuple(range(2 + 2 * len(shifts)))
    xs = [own[last], to_near(own[last])]
    tail = part(xs, places[:2], weight, bias)
    for k in range(last):
        xs = {0: own[k], 1: to_near(own[k])}
        for place, got in zip(places[2::2], arrived[k]):
            xs[place], xs[place + 1] = got, to_near(got)
        wanted, base = places, bias
        if k >= last - SPLIT:
            wanted = places[3::2]
            held = tuple(p for p in places if p not in wanted)
            base = part([xs[p] for p in held], held, weight, bias)
        xs = [xs[p] for p in wanted]
        if k < last - 1:
            out = layer(xs, wanted, weight, base, out, firsts[k] * unit, rows)
    return finish(xs, arrived[last], crossed, weight, base, tail, out)


def solution(mesh):
    placed = (P("dp", "feat"), P("feat"), P("feat"), P(None, "feat"), P("feat"))
    return jax.shard_map(local, mesh=mesh, in_specs=placed, out_specs=P("dp", "feat"), check_vma=False)
```

```python
import functools

import jax
import jax.numpy as jnp
from jax import lax
from jax.experimental import pallas as pl
from jax.experimental.pallas import tpu as pltpu
from jax.sharding import PartitionSpec as P


UNITS = 96
EARLY = (8, 20)
LATE = (31, 17, 9, 5, 4)
DIRECT = 2
PIECE = 10
SPLIT = 3
CROSSED = (5, 6)


def grant(kib):
    return pltpu.CompilerParams(vmem_limit_bytes=kib * 1024)


def centre_kernel(x_ref, sent_ref, mean_ref, buf, sem):
    copy = pltpu.make_async_copy(x_ref.at[pl.ds(0, buf.shape[0]), :], buf, sem)
    copy.start()
    copy.wait()
    x = buf[...]
    mean = jnp.mean(x, axis=0, keepdims=True)
    sent_ref[...] = (x - mean).astype(jnp.bfloat16)
    mean_ref[...] = mean


def centre(features, count):
    cols = features.shape[1]
    return pl.pallas_call(
        centre_kernel,
        in_specs=[pl.BlockSpec(memory_space=pltpu.HBM)],
        out_specs=[pl.BlockSpec(memory_space=pltpu.VMEM)] * 2,
        out_shape=[
            jax.ShapeDtypeStruct((count, cols), jnp.bfloat16),
            jax.ShapeDtypeStruct((1, cols), jnp.float32),
        ],
        scratch_shapes=[pltpu.VMEM((count, cols), jnp.float32), pltpu.SemaphoreType.DMA],
        compiler_params=grant(51000),
    )(features)


def survey_kernel(x_ref, pivot_ref, held_ref, sent_ref, means_ref, total_ref, sems, *, early, others):
    rows, cols = held_ref.shape
    copies = []
    for p, (start, size) in enumerate(early + others):
        place = pl.ds(start, size)
        copies.append(pltpu.make_async_copy(x_ref.at[place, :], held_ref.at[place, :], sems.at[p]))
        copies[-1].start()
    pivot = pivot_ref[...]
    groups = []
    for p, (start, size) in enumerate(early):
        copies[p].wait()
        x = held_ref[pl.ds(start, size), :]
        mean = jnp.mean(x, axis=0, keepdims=True)
        d = x - mean
        sent_ref[pl.ds(start - early[0][0], size), :] = d.astype(jnp.bfloat16)
        means_ref[pl.ds(p, 1), :] = mean
        groups.append((size, mean, jnp.sum(d * d, axis=0, keepdims=True)))
    sums = jnp.zeros((8, cols), jnp.float32)
    devs = jnp.zeros((8, cols), jnp.float32)
    rest = 0
    for p, (start, size) in enumerate(others, len(early)):
        copies[p].wait()
        d = (held_ref[pl.ds(start, size), :] - pivot).reshape(-1, 8, cols)
        sums = sums + jnp.sum(d, axis=0)
        devs = devs + jnp.sum(d * d, axis=0)
        rest += size
    shift = jnp.sum(sums, axis=0, keepdims=True) / rest
    dev = jnp.sum(devs, axis=0, keepdims=True) - rest * (shift * shift)
    groups.append((rest, pivot + shift, dev))
    mean = sum(n * m for n, m, _ in groups) / rows
    dev = sum(d + n * ((m - mean) * (m - mean)) for n, m, d in groups)
    total_ref[0:1, :] = mean
    total_ref[1:2, :] = dev


def survey(features, pivot, first, early, piece):
    rows, cols = features.shape
    pieces = tuple((first + p, piece) for p in range(0, early, piece))
    others = tuple((p, min(2 * piece, rows - p)) for p in range(first + early, rows, 2 * piece)) + ((0, first),)
    return pl.pallas_call(
        functools.partial(survey_kernel, early=pieces, others=others),
        in_specs=[pl.BlockSpec(memory_space=pltpu.HBM), pl.BlockSpec(memory_space=pltpu.VMEM)],
        out_specs=[pl.BlockSpec(memory_space=pltpu.VMEM)] * 4,
        out_shape=[
            jax.ShapeDtypeStruct((rows, cols), jnp.float32),
            jax.ShapeDtypeStruct((early, cols), jnp.bfloat16),
            jax.ShapeDtypeStruct((early // piece, cols), jnp.float32),
            jax.ShapeDtypeStruct((2, cols), jnp.float32),
        ],
        scratch_shapes=[pltpu.SemaphoreType.DMA((len(pieces) + len(others),))],
        compiler_params=grant(46000),
    )(features, pivot)


def shard_order():
    feat = lax.axis_size("feat")
    me = lax.axis_index("feat")
    order = [me, me ^ 1]
    for s in range(2, feat, 2):
        source = (me - s) % feat
        order += [source, source ^ 1]
    return order


def weights_of(w_ref, place, cols):
    return w_ref[pl.ds(pl.multiple_of(shard_order()[place] * cols, cols), cols), :]


def product(xs, places, w_ref, total):
    for x, place in zip(xs, places):
        w = weights_of(w_ref, place, x.shape[1])
        total = total + jnp.dot(x, w, preferred_element_type=jnp.float32)
    return total


def part_kernel(*refs, places):
    n = len(places)
    xs, (w_ref, bias_ref, out_ref) = refs[:n], refs[n:]
    out_ref[...] = product([x[...] for x in xs], places, w_ref, bias_ref[...])


def part(xs, places, weight, bias):
    return pl.pallas_call(
        functools.partial(part_kernel, places=places),
        in_specs=[pl.BlockSpec(memory_space=pltpu.VMEM)] * (len(xs) + 2),
        out_specs=pl.BlockSpec(memory_space=pltpu.VMEM),
        out_shape=jax.ShapeDtypeStruct((xs[0].shape[0], weight.shape[1]), jnp.float32),
        compiler_params=grant(12288),
    )(*xs, weight, bias)


def layer_kernel(*refs, places, first, blocks):
    n = len(places)
    xs, (w_ref, base_ref) = refs[:n], refs[n : n + 2]
    out_ref, buf, sems = refs[-3:]
    copies = []
    for b, (start, size) in enumerate(blocks):
        rows = pl.ds(start, size)
        base = base_ref[...] if base_ref.shape[0] == 1 else base_ref[rows, :]
        buf[rows, :] = jnp.maximum(product([x[rows, :] for x in xs], places, w_ref, base), 0.0)
        copies.append(pltpu.make_async_copy(buf.at[rows, :], out_ref.at[pl.ds(first + start, size), :], sems.at[b]))
        copies[-1].start()
    for copy in copies:
        copy.wait()


def layer(xs, places, weight, base, out, first, rows):
    count = xs[0].shape[0]
    width = weight.shape[1]
    blocks = tuple((start, min(256, count - start)) for start in range(0, count, 256))
    in_specs = [pl.BlockSpec(memory_space=pltpu.VMEM)] * (len(xs) + 2)
    args = [*xs, weight, base]
    aliases = {}
    if out is not None:
        in_specs += [pl.BlockSpec(memory_space=pltpu.HBM)]
        aliases = {len(args): 0}
        args += [out]
    return pl.pallas_call(
        functools.partial(layer_kernel, places=places, first=first, blocks=blocks),
        in_specs=in_specs,
        out_specs=pl.BlockSpec(memory_space=pltpu.HBM),
        out_shape=jax.ShapeDtypeStruct((rows, width), jnp.float32),
        input_output_aliases=aliases,
        scratch_shapes=[pltpu.VMEM((count, width), jnp.float32), pltpu.SemaphoreType.DMA((len(blocks),))],
        compiler_params=grant(12288),
    )(*args)


def finish_kernel(*refs, shifts, held):
    passed, far, cross = refs[:shifts], refs[shifts : 2 * shifts], refs[2 * shifts : 3 * shifts]
    w_ref, base_ref, tail_ref, _, out_ref, buf, sem = refs[3 * shifts :]
    count = buf.shape[0]
    tail = product([x[...] for x in far], range(held, held + 2 * shifts, 2), w_ref, tail_ref[...])
    xs = [jnp.concatenate([p[...], c[...]]) for p, c in zip(passed, cross)]
    base = jnp.concatenate([base_ref[...], tail])
    buf[...] = jnp.maximum(product(xs, range(5 - held, 5 - held + 2 * shifts, 2), w_ref, base), 0.0)
    copy = pltpu.make_async_copy(buf, out_ref.at[pl.ds(out_ref.shape[0] - count, count), :], sem)
    copy.start()
    copy.wait()


def finish(passed, far, cross, held, weight, base, tail, out):
    count = base.shape[0] + tail.shape[0]
    vmem = 3 * len(passed) + 3
    return pl.pallas_call(
        functools.partial(finish_kernel, shifts=len(passed), held=held),
        in_specs=[pl.BlockSpec(memory_space=pltpu.VMEM)] * vmem + [pl.BlockSpec(memory_space=pltpu.HBM)],
        out_specs=pl.BlockSpec(memory_space=pltpu.HBM),
        out_shape=jax.ShapeDtypeStruct(out.shape, out.dtype),
        input_output_aliases={vmem: 0},
        scratch_shapes=[pltpu.VMEM((count, weight.shape[1]), jnp.float32), pltpu.SemaphoreType.DMA],
        compiler_params=grant(12288),
    )(*passed, *far, *cross, weight, base, tail, out)


def local(features, gamma, beta, weight, bias):
    rows, cols = features.shape
    dp = lax.axis_size("dp")
    feat = lax.axis_size("feat")
    unit = rows // UNITS
    total_rows = rows * dp
    near = [(i, i ^ 1) for i in range(feat)]
    shifts = range(2, feat, 2)

    def to_far(x):
        return [lax.ppermute(x, "feat", [(i, (i + s) % feat) for i in range(feat)]) for s in shifts]

    def to_cross(x):
        return [lax.ppermute(x, "feat", [(i, (i + s) % feat ^ 1) for i in range(feat)]) for s in shifts]

    def to_near(x):
        return lax.ppermute(x, "feat", near)

    firsts = [0]
    for count in EARLY + LATE + (DIRECT,):
        firsts.append(firsts[-1] + count)
    piece = PIECE * unit
    sizes = [EARLY[0] * unit, piece]
    sent, pivot = centre(features, EARLY[0] * unit)
    early = [to_far(sent)]
    features, sent, means, mine = survey(features, pivot, EARLY[0] * unit, EARLY[1] * unit, piece)
    early.append(to_far(sent))
    found = [pivot, means]
    step, held = 1, rows
    while step < dp:
        theirs = lax.ppermute(mine, "dp", [(i, i ^ step) for i in range(dp)])
        gap = mine[0] - theirs[0]
        mean = (mine[0] + theirs[0]) * 0.5
        dev = mine[1] + theirs[1] + (0.5 * held) * (gap * gap)
        mine = jnp.stack([mean, dev])
        step, held = 2 * step, 2 * held
    mean = mine[0]
    var = mine[1] / total_rows
    scale = gamma / jnp.sqrt(var + 1e-05)

    def normalize(k):
        x = features[firsts[k] * unit : firsts[k + 1] * unit]
        return ((x - mean) * scale + beta).astype(jnp.bfloat16)

    own, arrived = {}, {}
    last = len(EARLY) + len(LATE)
    for k in range(len(EARLY), last + 1):
        own[k] = normalize(k)
        arrived[k] = (to_cross if k in CROSSED else to_far)(own[k])
    crossed = to_cross(own[last])
    offsets = (jnp.concatenate(found) - mean) * scale + beta
    table = to_far(jnp.concatenate([scale[None], offsets]))
    row = 1
    for k, means in enumerate(found):
        own[k] = normalize(k)
        arrived[k] = []
        blocks = means.shape[0]
        for got, t in zip(early[k], table):
            got = got.reshape(blocks, sizes[k], cols).astype(jnp.float32)
            got = got * t[0] + t[row : row + blocks][:, None, :]
            arrived[k].append(got.astype(jnp.bfloat16).reshape(blocks * sizes[k], cols))
        row += blocks

    out = None
    bias = bias[None]
    places = tuple(range(2 + 2 * len(shifts)))
    xs = [own[last], to_near(own[last])]
    tail = part(xs, places[:2], weight, bias)
    for k in range(last):
        xs = {0: own[k], 1: to_near(own[k])}
        for place, got in zip(places[2::2], arrived[k]):
            xs[place], xs[place + 1] = (to_near(got), got) if k in CROSSED else (got, to_near(got))
        wanted, base = places, bias
        if k >= last - SPLIT:
            wanted = places[2::2] if k in CROSSED else places[3::2]
            held = tuple(p for p in places if p not in wanted)
            base = part([xs[p] for p in held], held, weight, bias)
        xs = [xs[p] for p in wanted]
        if k < last - 1:
            out = layer(xs, wanted, weight, base, out, firsts[k] * unit, rows)
    ends = (crossed, arrived[last], 3) if last - 1 in CROSSED else (arrived[last], crossed, 2)
    return finish(xs, *ends, weight, base, tail, out)


def solution(mesh):
    placed = (P("dp", "feat"), P("feat"), P("feat"), P(None, "feat"), P("feat"))
    return jax.shard_map(local, mesh=mesh, in_specs=placed, out_specs=P("dp", "feat"), check_vma=False)
```
